32 devices in a mesh: dp: 4 (over z), expert: 2 (over x), tensor: 4 (over y, core).
Axes of the slice: x: 2, y: 2, z: 4, core: 2. Of those that a mesh axis runs over, the one named last changes fastest.
Arguments:
- tokens: bfloat16 [256, 4096], P(('dp', 'expert', 'tensor')), may hold values from -6 to 6
- out_grad: bfloat16 [256, 4096], P(('dp', 'expert', 'tensor')), may hold values from -4 to 4
- route_probs: float32 [256, 2], P(('dp', 'expert')), may hold values from 0.2 to 1
- expert_ids: int32 [256, 2], P(('dp', 'expert')), may hold values from 0 to 7, as said below
- slot_index: int32 [256, 2], P(('dp', 'expert')), may hold values from 0 to 10, as said below
- w_gate: bfloat16 [8, 4096, 7168], P('expert', 'dp', 'tensor'), may hold values from -0.09375 to 0.09375
- w_up: bfloat16 [8, 4096, 7168], P('expert', 'dp', 'tensor'), may hold values from -0.09375 to 0.09375
- w_down: bfloat16 [8, 7168, 4096], P('expert', 'tensor', 'dp'), may hold values from -0.0625 to 0.0625
Outputs:
- token_grad: bfloat16 [256, 4096], P(('dp', 'expert', 'tensor'))
- grad_gate: bfloat16 [8, 4096, 7168], P('expert', 'dp', 'tensor')
- grad_up: bfloat16 [8, 4096, 7168], P('expert', 'dp', 'tensor')
- grad_down: bfloat16 [8, 7168, 4096], P('expert', 'tensor', 'dp')
The draws below stay inside these ranges and needn't reach their ends.
Inputs may be any that keep to these rules, and one draw needn't show every extreme that they name: `expert_ids`: the 2 entries of a token are different experts. slot_index[t, k] counts the earlier routes to expert_ids[t, k] within the token's routing block of 32 rows, in order of tokens and then of routes; the value 10 marks a route past the capacity, which is dropped (a count of 10 or more is given as 10). In every draw some expert is filled to 10 slots in every block.
All inputs are finite; a program needn't handle non-finite values.
Results may differ from the reference program's by a relative error of at most 0.011.
Values may be sent and summed in bfloat16 or wider, within the bound.
A program may use at most 192 MiB of HBM per device.

```python
import jax
import jax.numpy as jnp
from jax import lax

D = 4096
EXPERTS = 8
TOP = 2
FF = 7168
GROUP = 32
CAP = 10
TOKENS = 256


def route_draw(key):
    blocks = TOKENS // GROUP
    base = jax.random.fold_in(key, 7)
    hot_key, pick_key, first_key, second_key = jax.random.split(base, 4)
    hot_expert = jax.random.randint(hot_key, (), 0, EXPERTS)
    pick = jax.random.randint(pick_key, (blocks, GROUP), 0, 2)
    first_any = jax.random.randint(first_key, (blocks, GROUP), 0, EXPERTS)
    first = jnp.where(pick == 1, hot_expert, first_any)
    second = (first + 1 + jax.random.randint(second_key, (blocks, GROUP), 0, EXPERTS - 1)) % EXPERTS
    chosen = jnp.stack([first, second], -1).astype(jnp.int32)
    flat_ids = chosen.reshape(blocks, GROUP * TOP)
    onehot = (flat_ids[:, :, None] == jnp.arange(EXPERTS, dtype=jnp.int32)[None, None, :]).astype(jnp.int32)
    earlier = jnp.cumsum(onehot, axis=1) - onehot
    position = jnp.sum(earlier * onehot, axis=-1)
    position = jnp.minimum(position, CAP).astype(jnp.int32)
    return (chosen.reshape(TOKENS, TOP), position.reshape(TOKENS, TOP))


def draw_expert_ids(key, part):
    return route_draw(key)[0]


def draw_slot_index(key, part):
    return route_draw(key)[1]


def level_of(rng, shape, cuts, low, largest):
    def one(axis_at, blocks):
        steps = jax.random.uniform(jax.random.fold_in(jax.random.fold_in(rng, 6), axis_at), (blocks,), jnp.float32, low / len(cuts), largest / len(cuts))
        return jnp.repeat(jnp.exp(steps), shape[axis_at] // blocks).reshape((-1,) + (1,) * (len(shape) - axis_at - 1))

    gain = one(*cuts[0])
    for cut in cuts[1:]:
        gain = gain * one(*cut)
    return gain


def scatter_about(own_key, extent, spread, most, cuts=(), kind=jnp.bfloat16):
    values = jax.random.normal(own_key, extent, jnp.float32) * spread
    if len(cuts) > 0:
        values = level_of(own_key, extent, cuts, -0.22, 0.18) * values
    return jnp.clip(values, min=-most, max=most).astype(kind)


def setup_inputs(seed: int = 0) -> dict:
    key_of = jax.random.split(jax.random.key(seed), 9)
    return {
        "tokens": scatter_about(key_of[0], (TOKENS, D), 1.0, 6.0, ((0, 32),)),
        "out_grad": scatter_about(key_of[1], (TOKENS, D), 0.5, 4.0, ((0, 32),)),
        "route_probs": jnp.clip(0.2 + 0.8 * jax.random.uniform(key_of[2], (TOKENS, TOP), jnp.float32) ** level_of(key_of[2], (TOKENS, TOP), ((0, 8),), -0.2, 0.2), 0.2, 1.0),
        "expert_ids": draw_expert_ids(jax.random.fold_in(key_of[8], 71), 0),
        "slot_index": draw_slot_index(jax.random.fold_in(key_of[8], 71), 0),
        "w_gate": scatter_about(key_of[5], (EXPERTS, D, FF), D ** -0.5, 0.09375, ((0, 2), (1, 4), (2, 4))),
        "w_up": scatter_about(key_of[6], (EXPERTS, D, FF), D ** -0.5, 0.09375, ((0, 2), (1, 4), (2, 4))),
        "w_down": scatter_about(key_of[7], (EXPERTS, FF, D), FF ** -0.5, 0.0625, ((0, 2), (1, 4), (2, 4))),
    }


def route_tables(expert_ids, slot_index, capacity):
    target = slot_index * EXPERTS + expert_ids
    target = jnp.where(slot_index < capacity, target, -1).astype(jnp.int32)
    places = jnp.arange(capacity * EXPERTS, dtype=jnp.int32)
    return [(places[:, None] == target[None, :, k]).astype(jnp.bfloat16) for k in range(TOP)]


def swiglu_back(pre_gate, pre_up, grad_hidden):
    sigmoid_gate = jax.nn.sigmoid(pre_gate)
    silu_gate = pre_gate * sigmoid_gate
    hidden = (silu_gate * pre_up).astype(jnp.bfloat16)
    up_delta = (grad_hidden * silu_gate).astype(jnp.bfloat16)
    gate_delta = (grad_hidden * pre_up * sigmoid_gate * (1.0 + pre_gate * (1.0 - sigmoid_gate))).astype(jnp.bfloat16)
    return hidden, gate_delta, up_delta


def reference(tokens, out_grad, route_probs, expert_ids, slot_index, w_gate, w_up, w_down):
    blocks = TOKENS // GROUP
    capacity = CAP

    def dispatch(inputs):
        block_x, block_dy, block_probs, block_ids, block_slots = inputs
        tables = route_tables(block_ids, block_slots, capacity)
        table_sum = tables[0] + tables[1]
        x_buf = jnp.dot(table_sum, block_x, preferred_element_type=jnp.float32).astype(jnp.bfloat16)
        grad_buf = jnp.zeros((capacity * EXPERTS, D), jnp.float32)
        for k in range(TOP):
            scaled = (block_probs[:, k:k + 1] * block_dy.astype(jnp.float32)).astype(jnp.bfloat16)
            grad_buf = grad_buf + jnp.dot(tables[k], scaled, preferred_element_type=jnp.float32)
        grad_buf = grad_buf.astype(jnp.bfloat16)
        return (x_buf.reshape(capacity, EXPERTS, D), grad_buf.reshape(capacity, EXPERTS, D),
                table_sum.astype(jnp.float32))

    x_bufs, grad_bufs, table_all = lax.map(dispatch, (
        tokens.reshape(blocks, GROUP, D), out_grad.reshape(blocks, GROUP, D),
        route_probs.reshape(blocks, GROUP, TOP), expert_ids.reshape(blocks, GROUP, TOP),
        slot_index.reshape(blocks, GROUP, TOP)))
    expert_x = jnp.moveaxis(x_bufs, 2, 0).reshape(EXPERTS, blocks * capacity, D)
    expert_g = jnp.moveaxis(grad_bufs, 2, 0).reshape(EXPERTS, blocks * capacity, D)

    def expert_back(inputs):
        rows_x, rows_g, gate_w, up_w, down_w = inputs
        pre_gate = jnp.dot(rows_x, gate_w, preferred_element_type=jnp.float32)
        pre_up = jnp.dot(rows_x, up_w, preferred_element_type=jnp.float32)
        grad_hidden = jnp.dot(rows_g, down_w.T, preferred_element_type=jnp.float32)
        hidden, gate_delta, up_delta = swiglu_back(pre_gate, pre_up, grad_hidden)
        g_down = jnp.dot(hidden.T, rows_g, preferred_element_type=jnp.float32).astype(jnp.bfloat16)
        g_gate = jnp.dot(rows_x.T, gate_delta, preferred_element_type=jnp.float32).astype(jnp.bfloat16)
        g_up = jnp.dot(rows_x.T, up_delta, preferred_element_type=jnp.float32).astype(jnp.bfloat16)
        row_grad = jnp.dot(gate_delta, gate_w.T, preferred_element_type=jnp.float32)
        row_grad = row_grad + jnp.dot(up_delta, up_w.T, preferred_element_type=jnp.float32)
        return g_gate, g_up, g_down, row_grad

    grad_gate, grad_up, grad_down, row_grad = lax.map(expert_back, (expert_x, expert_g, w_gate, w_up, w_down))
    row_grad = row_grad.reshape(EXPERTS, blocks, capacity, D)
    row_grad = jnp.transpose(row_grad, (1, 2, 0, 3)).reshape(blocks, capacity * EXPERTS, D)
    token_grad = jnp.einsum("bjt,bjd->btd", table_all, row_grad, precision=lax.Precision.HIGHEST)
    token_grad = token_grad.reshape(TOKENS, D).astype(jnp.bfloat16)
    return token_grad, grad_gate, grad_up, grad_down
```

```python
import functools

import jax
import jax.numpy as jnp
from jax import lax
from jax.experimental import pallas as pl
from jax.experimental.pallas import tpu as pltpu
from jax.sharding import PartitionSpec as P

EXPERTS = 8
TOP = 2
BF = jnp.bfloat16
F32 = jnp.float32


def swiglu_back(pre_gate, pre_up, grad_hidden):
    sigmoid_gate = jax.nn.sigmoid(pre_gate)
    silu_gate = pre_gate * sigmoid_gate
    hidden = (silu_gate * pre_up).astype(BF)
    up_delta = (grad_hidden * silu_gate).astype(BF)
    gate_delta = (
        grad_hidden * pre_up * sigmoid_gate * (1.0 + pre_gate * (1.0 - sigmoid_gate))
    ).astype(BF)
    return (hidden, gate_delta, up_delta)


def dot(spec, a, b):
    return jnp.einsum(spec, a, b, preferred_element_type=F32)


def ring_kernel(n, gate, up, down, hidden, gate_delta, up_delta, land, *sems):
    sum_send, sum_recv, out_send, out_recv = sems
    me = lax.axis_index("dp")
    right, left = lax.rem(me + 1, n), lax.rem(me + n - 1, n)
    parts, outs = (gate, up, down), (hidden, gate_delta, up_delta)
    rows, width = gate.shape[1:]
    cut = width // 256 * 128
    columns = (pl.ds(0, cut), pl.ds(cut, width - cut))
    to = (right, left)
    step_rows = 16
    every = [(d, m) for m in range(3) for d in range(2)]

    def chunk(d, back):
        return lax.rem(me + 2 * n - back, n) if d == 0 else lax.rem(me + back, n)

    def sum_copy(s, d, m):
        if s == 0:
            src = parts[m].at[chunk(d, 1), :, columns[d]]
        else:
            src = land.at[s - 1, m, :, columns[d]]
        return pltpu.make_async_remote_copy(
            src_ref=src,
            dst_ref=land.at[s, m, :, columns[d]],
            send_sem=sum_send.at[s, d, m],
            recv_sem=sum_recv.at[s, d, m],
            device_id={"dp": to[d]},
            device_id_type=pl.DeviceIdType.MESH,
        )

    def out_copy(s, d, m):
        piece = outs[m].at[chunk(d, s), :, columns[d]]
        return pltpu.make_async_remote_copy(
            src_ref=piece,
            dst_ref=piece,
            send_sem=out_send.at[s, d, m],
            recv_sem=out_recv.at[s, d, m],
            device_id={"dp": to[d]},
            device_id_type=pl.DeviceIdType.MESH,
        )

    barrier = pltpu.get_barrier_semaphore()
    for other in to:
        pl.semaphore_signal(
            barrier, inc=1, device_id={"dp": other}, device_id_type=pl.DeviceIdType.MESH
        )
    pl.semaphore_wait(barrier, 2)

    for d, m in every:
        sum_copy(0, d, m).start()
    for s in range(n - 2):
        for d, m in every:
            sum_copy(s, d, m).wait_recv()
            at = chunk(d, s + 2)

            @pl.loop(0, rows // step_rows)
            def _(i):
                r = pl.ds(pl.multiple_of(i * step_rows, step_rows), step_rows)
                own = parts[m][at, r, columns[d]].astype(F32)
                land[s, m, r, columns[d]] = (
                    land[s, m, r, columns[d]].astype(F32) + own
                ).astype(BF)

            sum_copy(s + 1, d, m).start()
    for d in range(2):
        for m in range(3):
            sum_copy(n - 2, d, m).wait_recv()

        @pl.loop(0, rows // step_rows)
        def _(i):
            r = pl.ds(pl.multiple_of(i * step_rows, step_rows), step_rows)
            values = [
                land[n - 2, m, r, columns[d]].astype(F32)
                + parts[m][me, r, columns[d]].astype(F32)
                for m in range(3)
            ]
            for ref, value in zip(outs, swiglu_back(*values)):
                ref[me, r, columns[d]] = value

        for m in range(3):
            out_copy(0, d, m).start()
    for s in range(n - 1):
        for d, m in every:
            out_copy(s, d, m).wait_recv()
            if s < n - 2:
                out_copy(s + 1, d, m).start()
    for s in range(n - 1):
        for d, m in every:
            sum_copy(s, d, m).wait_send()
            out_copy(s, d, m).wait_send()


def ring_back(pre_gate, pre_up, grad_hidden):
    n = lax.axis_size("dp")
    rows, width = pre_gate.shape[0] // n, pre_gate.shape[1]
    shape = jax.ShapeDtypeStruct((n, rows, width), BF)
    spec = pl.BlockSpec(memory_space=pltpu.VMEM)
    sems = pltpu.SemaphoreType.DMA((n - 1, 2, 3))
    return pl.pallas_call(
        functools.partial(ring_kernel, n),
        out_shape=[shape] * 3,
        in_specs=[spec] * 3,
        out_specs=[spec] * 3,
        scratch_shapes=[pltpu.VMEM((n - 1, 3, rows, width), BF), sems, sems, sems, sems],
        compiler_params=pltpu.CompilerParams(
            collective_id=0, has_side_effects=True, vmem_limit_bytes=40 * 2**20
        ),
    )(*[v.reshape(n, rows, width) for v in (pre_gate, pre_up, grad_hidden)])


def shards(tokens, out_grad, route_probs, expert_ids, slot_index, w_gate, w_up, w_down):
    n_dp, n_ex, n_tn = lax.axis_size("dp"), lax.axis_size("expert"), lax.axis_size("tensor")
    rows, width = tokens.shape
    piece = width // n_dp
    block_rows = rows * n_tn
    blocks = n_dp * n_ex
    everyone = blocks * block_rows
    capacity = 5 * block_rows * TOP // (4 * EXPERTS)
    local_experts = w_gate.shape[0]
    hidden_width = w_gate.shape[2]
    slots = blocks * capacity

    both = jnp.concatenate([tokens, out_grad], 0)
    both = both.reshape(2 * rows, n_dp, piece).transpose(1, 0, 2)
    both = lax.all_to_all(both, "dp", split_axis=0, concat_axis=0, tiled=True)
    both = lax.all_gather(both, ("expert", "tensor"), axis=0, tiled=False)
    x_all = both[:, :, :rows].reshape(everyone, piece)
    g_all = both[:, :, rows:].reshape(everyone, piece)

    routes = jnp.concatenate(
        [expert_ids.astype(F32), slot_index.astype(F32), route_probs], axis=1
    )
    routes = lax.all_gather(routes, ("dp", "expert"), axis=0, tiled=True)
    routes = routes.reshape(n_dp, n_ex, n_tn, rows, 3 * TOP)
    routes = routes.transpose(4, 1, 2, 0, 3).reshape(3 * TOP, everyone)
    ids = routes[:TOP].astype(jnp.int32)
    slot = routes[TOP : 2 * TOP].astype(jnp.int32)
    probs = routes[2 * TOP :]
    at = jnp.arange(everyone, dtype=jnp.int32)
    block = (at // rows) % n_dp * n_ex + at // (rows * n_dp * n_tn)
    mine = ids - lax.axis_index("expert") * local_experts
    kept = (slot < capacity) & (mine >= 0) & (mine < local_experts)
    target = jnp.where(kept, mine * slots + block[None] * capacity + slot, -1)
    places = jnp.arange(local_experts * slots, dtype=jnp.int32)
    hits = [places[:, None] == target[k][None] for k in range(TOP)]
    table = sum(h.astype(F32) for h in hits).astype(BF)
    slot_prob = sum(
        jnp.sum(jnp.where(hits[k], probs[k][None], 0.0), axis=1) for k in range(TOP)
    )
    token_rows = dot("st,td->sd", table, x_all).astype(BF)
    grad_rows = (dot("st,td->sd", table, g_all) * slot_prob[:, None]).astype(BF)
    token_rows = token_rows.reshape(local_experts, slots, piece)
    grad_rows = grad_rows.reshape(local_experts, slots, piece)

    def flat(value):
        return value.astype(BF).reshape(local_experts * slots, hidden_width)

    together = ring_back(
        flat(dot("lsd,ldf->lsf", token_rows, w_gate)),
        flat(dot("lsd,ldf->lsf", token_rows, w_up)),
        flat(dot("lsd,lfd->lsf", grad_rows, w_down)),
    )
    hidden, gate_delta, up_delta = [
        v.reshape(local_experts, slots, hidden_width) for v in together
    ]

    row_grad = dot("lsf,ldf->lsd", gate_delta, w_gate) + dot("lsf,ldf->lsd", up_delta, w_up)
    row_grad = row_grad.astype(BF).reshape(local_experts * slots, piece)
    token_part = dot("st,sd->td", table, row_grad).astype(BF)
    token_grad = lax.psum_scatter(
        token_part, ("expert", "tensor"), scatter_dimension=0, tiled=True
    )
    token_grad = token_grad.reshape(n_dp, rows, piece)
    token_grad = lax.all_to_all(token_grad, "dp", split_axis=0, concat_axis=0, tiled=True)
    token_grad = token_grad.transpose(1, 0, 2).reshape(rows, width)

    grad_gate = dot("lsd,lsf->ldf", token_rows, gate_delta).astype(BF)
    grad_up = dot("lsd,lsf->ldf", token_rows, up_delta).astype(BF)
    grad_down = dot("lsf,lsd->lfd", hidden, grad_rows).astype(BF)
    return (token_grad, grad_gate, grad_up, grad_down)


def solution(mesh):
    placed = (
        P(("dp", "expert", "tensor"), None),
        P(("dp", "expert", "tensor"), None),
        P(("dp", "expert"), None),
        P(("dp", "expert"), None),
        P(("dp", "expert"), None),
        P("expert", "dp", "tensor"),
        P("expert", "dp", "tensor"),
        P("expert", "tensor", "dp"),
    )
    return jax.shard_map(
        shards,
        mesh=mesh,
        in_specs=placed,
        out_specs=(
            P(("dp", "expert", "tensor"), None),
            P("expert", "dp", "tensor"),
            P("expert", "dp", "tensor"),
            P("expert", "tensor", "dp"),
        ),
        check_vma=False,
    )
```
